32 devices in a mesh: batch: 4 (over y, z), time: 8 (over x, core).
Axes of the slice: x: 4, y: 2, z: 2, core: 2. Of those that a mesh axis runs over, the one named last changes fastest.
The devices are a block of a 4x4x8 slice.
Arguments:
- latent: bfloat16 [64, 6, 128, 384], P(('batch', 'time')), parts along dimension 0
- conv_w: bfloat16 [4, 3, 3, 3, 384, 384], replicated
- conv_b: float32 [4, 384], replicated
- norm_g: float32 [5, 384], replicated
- norm_b: float32 [5, 384], replicated
- attn_w: bfloat16 [4, 384, 384], replicated
- attn_b: float32 [4, 384], replicated
Outputs:
- output: bfloat16 [64, 6, 128, 384], P(('batch', 'time')), parts along dimension 0
There are 4 independent parts. The reference program is written for one: setup_inputs(seed, part) draws one part's arguments, and reference() takes and returns one part's arrays. A program takes and returns all parts, laid end to end along the dimension named above; an argument that names none is the same for every part.
All inputs are finite; a program needn't handle non-finite values.
Results may differ from the reference program's by a relative error of at most 0.0124883.
Values are sent between devices in bfloat16 or wider.
A program may use at most 768 MiB of HBM per device.

```python
import jax
import jax.numpy as jnp
from jax import lax

FRAMES = 16
HEIGHT = 6
WIDTH = 128
CHANNELS = 384
GROUPS = 32
NORM_EPS = 1e-6


def setup_inputs(seed: int = 0, part: int = 0) -> dict:
    part_key = jax.random.fold_in(jax.random.key(seed), part)
    video_keys = jax.random.split(part_key, 4)
    weight_keys = jax.random.split(jax.random.key(seed + 1), 6)
    time_pos = jnp.arange(FRAMES, dtype=jnp.float32) / max(FRAMES - 1, 1) - 0.5
    time_slope = 1.4 + 0.4 * jax.random.uniform(video_keys[0], (), jnp.float32)
    frame_scale = jnp.exp(time_slope * time_pos)[:, None, None, None]
    chan_offset = jax.random.normal(video_keys[1], (CHANNELS,), jnp.float32)
    frame_mean = time_pos[:, None, None, None] * chan_offset
    shared_noise = jax.random.normal(video_keys[2], (1, HEIGHT, WIDTH, CHANNELS), jnp.float32)
    fresh_noise = jax.random.normal(video_keys[3], (FRAMES, HEIGHT, WIDTH, CHANNELS), jnp.float32)
    latent = frame_scale * (0.5 * shared_noise + 0.85 * fresh_noise) + frame_mean
    conv_w = jax.random.normal(weight_keys[0], (4, 3, 3, 3, CHANNELS, CHANNELS), jnp.float32) * (27 * CHANNELS) ** -0.5
    conv_b = 0.3 * jax.random.normal(weight_keys[1], (4, CHANNELS), jnp.float32)
    norm_g = 1.0 + 0.3 * jax.random.normal(weight_keys[2], (5, CHANNELS), jnp.float32)
    norm_b = 0.3 * jax.random.normal(weight_keys[3], (5, CHANNELS), jnp.float32)
    attn_w = jax.random.normal(weight_keys[4], (4, CHANNELS, CHANNELS), jnp.float32) * CHANNELS ** -0.5
    attn_b = 0.3 * jax.random.normal(weight_keys[5], (4, CHANNELS), jnp.float32)
    return {"latent": latent.astype(jnp.bfloat16), "conv_w": conv_w.astype(jnp.bfloat16), "conv_b": conv_b, "norm_g": norm_g, "norm_b": norm_b, "attn_w": attn_w.astype(jnp.bfloat16), "attn_b": attn_b}


def group_norm(feature, norm_gain, norm_shift):
    values_f = feature.astype(jnp.float32)
    grouped = values_f.reshape(FRAMES, HEIGHT, WIDTH, GROUPS, CHANNELS // GROUPS)
    elem_count = FRAMES * HEIGHT * WIDTH * (CHANNELS // GROUPS)
    group_mean = jnp.sum(grouped, axis=(0, 1, 2, 4)) / elem_count
    group_sq = jnp.sum(grouped * grouped, axis=(0, 1, 2, 4)) / elem_count
    inv_std = lax.rsqrt(group_sq - group_mean * group_mean + NORM_EPS)
    mean_full = jnp.repeat(group_mean, CHANNELS // GROUPS)
    scale_full = jnp.repeat(inv_std, CHANNELS // GROUPS) * norm_gain
    return (values_f - mean_full) * scale_full + norm_shift


def causal_conv(activation, kernel, conv_bias):
    padded = jnp.concatenate([activation[:1], activation[:1], activation], axis=0)
    conv_out = lax.conv_general_dilated(padded[None].astype(jnp.float32), kernel.astype(jnp.float32), (1, 1, 1), ((0, 0), (1, 1), (1, 1)), dimension_numbers=("NDHWC", "DHWIO", "NDHWC"))
    return (conv_out[0] + conv_bias).astype(jnp.bfloat16)


def resnet_block(feature, conv_w, conv_b, norm_g, norm_b, norm_first, conv_first):
    activation = jax.nn.silu(group_norm(feature, norm_g[norm_first], norm_b[norm_first])).astype(jnp.bfloat16)
    branch = causal_conv(activation, conv_w[conv_first], conv_b[conv_first])
    activation = jax.nn.silu(group_norm(branch, norm_g[norm_first + 1], norm_b[norm_first + 1])).astype(jnp.bfloat16)
    branch = causal_conv(activation, conv_w[conv_first + 1], conv_b[conv_first + 1])
    return (feature.astype(jnp.float32) + branch.astype(jnp.float32)).astype(jnp.bfloat16)


def spatial_attention(feature, norm_gain, norm_shift, attn_w, attn_b):
    normed = group_norm(feature, norm_gain, norm_shift).astype(jnp.bfloat16)
    tokens = normed.reshape(FRAMES, HEIGHT * WIDTH, CHANNELS)
    score_scale = CHANNELS ** -0.5

    def one_frame(frame_tok):
        queries = (jnp.dot(frame_tok, attn_w[0], preferred_element_type=jnp.float32) + attn_b[0]).astype(jnp.bfloat16)
        keys_t = (jnp.dot(frame_tok, attn_w[1], preferred_element_type=jnp.float32) + attn_b[1]).astype(jnp.bfloat16)
        values_t = (jnp.dot(frame_tok, attn_w[2], preferred_element_type=jnp.float32) + attn_b[2]).astype(jnp.bfloat16)
        scores = jnp.dot(queries, keys_t.T, preferred_element_type=jnp.float32) * score_scale
        attn_probs = jax.nn.softmax(scores, axis=-1).astype(jnp.bfloat16)
        mixed_val = jnp.dot(attn_probs, values_t, preferred_element_type=jnp.float32).astype(jnp.bfloat16)
        return (jnp.dot(mixed_val, attn_w[3], preferred_element_type=jnp.float32) + attn_b[3]).astype(jnp.bfloat16)

    projected = lax.map(one_frame, tokens).reshape(feature.shape)
    return (feature.astype(jnp.float32) + projected.astype(jnp.float32)).astype(jnp.bfloat16)


def reference(latent, conv_w, conv_b, norm_g, norm_b, attn_w, attn_b):
    feature = resnet_block(latent, conv_w, conv_b, norm_g, norm_b, 0, 0)
    feature = spatial_attention(feature, norm_g[2], norm_b[2], attn_w, attn_b)
    return resnet_block(feature, conv_w, conv_b, norm_g, norm_b, 3, 2)
```

```python
import functools

import jax
import jax.numpy as jnp
from jax import lax
from jax.experimental import pallas as pl
from jax.experimental.pallas import tpu as pltpu
from jax.sharding import PartitionSpec as P

GROUPS = 32
NORM_EPS = 1e-6
CHUNK = 64
MESH = pl.DeviceIdType.MESH
F32 = jnp.float32
BF16 = jnp.bfloat16


def dot_t(lhs, rhs):
    return lax.dot_general(lhs, rhs, (((0,), (0,)), ((), ())), preferred_element_type=F32)


def kernel(ranks, height, width, x_hbm, w_hbm, conv_b, norm_g, norm_b, attn_w, attn_b, out_ref,
           x_in, w_buf, u_buf, acc, feat, halo, part, stat, coef, attn_q, attn_k, attn_v, attn_p,
           x_sem, w_sem, stat_send, stat_recv, halo_send, halo_recv):
    me = lax.axis_index("time")
    channels = feat.shape[2]
    per_group = channels // GROUPS
    elem_count = float(ranks * 2 * height * width * per_group)
    npos = height * width
    nchunk = channels // CHUNK
    k_tap = 3 * channels

    def x_copy():
        return pltpu.make_async_copy(x_hbm, x_in, x_sem)

    def w_copy(k, a):
        return pltpu.make_async_copy(w_hbm.at[k, a], w_buf.at[k % 2, a], w_sem.at[k % 2, a])

    def stat_copy(n, source, target):
        return pltpu.make_async_remote_copy(
            src_ref=stat.at[n, source], dst_ref=stat.at[n, source], send_sem=stat_send.at[n, target],
            recv_sem=stat_recv.at[n, source], device_id={"time": target}, device_id_type=MESH)

    def halo_copy(k, t):
        return pltpu.make_async_remote_copy(
            src_ref=feat.at[k % 2, t], dst_ref=halo.at[k, t], send_sem=halo_send.at[k, t],
            recv_sem=halo_recv.at[k, t], device_id={"time": lax.rem(me + 1, ranks)}, device_id_type=MESH)

    def start_halo(k):
        @pl.when(me < ranks - 1)
        def _():
            for t in (1, 0):
                halo_copy(k, t).start()

    def send_stats(n):
        rows = [jnp.sum(part[i].T, axis=0, keepdims=True) for i in range(2)]
        stat[n, me] = jnp.concatenate(rows, axis=0)
        for d in range(1, ranks):
            stat_copy(n, me, lax.rem(me + d, ranks)).start()

    def column(row):
        return jnp.broadcast_to(row, (128, channels)).T

    def norm_coefs(n):
        for d in range(1, ranks):
            stat_copy(n, lax.rem(me + d, ranks), lax.rem(me + d, ranks)).wait_recv()
        totals = jnp.sum(stat[n], axis=0)
        totals = jnp.concatenate([totals, jnp.zeros((6, channels), F32)], axis=0)
        magic = (65536 + per_group - 1) // per_group
        r = lax.broadcasted_iota(jnp.int32, (channels, channels), 0) * magic // 65536
        c = lax.broadcasted_iota(jnp.int32, (channels, channels), 1) * magic // 65536
        member = jnp.where(r == c, 1.0, 0.0).astype(F32)
        sums = jnp.dot(totals, member, precision=lax.Precision.HIGHEST, preferred_element_type=F32)
        mean = sums[0:1] / elem_count
        var = sums[1:2] / elem_count - mean * mean
        scale = lax.rsqrt(var + NORM_EPS) * norm_g[pl.ds(n, 1), :]
        coef[0] = column(mean)
        coef[1] = column(scale)
        coef[2] = column(norm_b[pl.ds(n, 1), :])
        for d in range(1, ranks):
            stat_copy(n, me, lax.rem(me + d, ranks)).wait_send()

    def normalize(value, c0):
        sl = pl.ds(c0, CHUNK)
        return (value.astype(F32) - coef[0, sl, :]) * coef[1, sl, :] + coef[2, sl, :]

    def fill_u(read, s):
        lane = lax.broadcasted_iota(jnp.int32, (CHUNK, width), 1)

        def body(ci, _):
            c0 = pl.multiple_of(ci * CHUNK, CHUNK)
            for i in range(height):
                half = 0.5 * normalize(read(c0, i), c0)
                u = half + half * jnp.tanh(half)
                left = jnp.where(lane == 0, 0.0, pltpu.roll(u, 1, 1))
                right = jnp.where(lane == width - 1, 0.0, pltpu.roll(u, width - 1, 1))
                cols = pl.ds((i + 1) * width, width)
                for e, v in enumerate((left, u, right)):
                    u_buf[s, pl.ds(e * channels + c0, CHUNK), cols] = v.astype(BF16)
            return 0

        lax.fori_loop(0, nchunk, body, 0)

    def taps(s):
        return jnp.concatenate([u_buf[s, :, pl.ds(d * width, npos)] for d in range(3)], axis=0)

    def frame_read(b, t):
        return lambda c0, i: feat[b, t, pl.ds(c0, CHUNK), pl.ds(i * width, width)]

    def halo_read(k, t):
        return lambda c0, i: halo[k, t, pl.ds(c0, CHUNK), pl.ds(i * width, width)]

    def get_halo(k, t):
        @pl.when(me > 0)
        def _():
            halo_copy(k, t).wait_recv()

        @pl.when(me == 0)
        def _():
            halo[k, t] = feat[k % 2, 0]

        fill_u(halo_read(k, t), t)

    def accumulate_stats(value_of):
        def body(ci, _):
            c0 = pl.multiple_of(ci * CHUNK, CHUNK)
            s1 = jnp.zeros((CHUNK, width), F32)
            s2 = jnp.zeros((CHUNK, width), F32)
            for t in range(2):
                for i in range(height):
                    v = value_of(t, c0, i)
                    s1 = s1 + v
                    s2 = s2 + v * v
            part[0, pl.ds(c0, CHUNK), :] = s1
            part[1, pl.ds(c0, CHUNK), :] = s2
            return 0

        lax.fori_loop(0, nchunk, body, 0)

    def attention():
        def norm_body(ci, _):
            c0 = pl.multiple_of(ci * CHUNK, CHUNK)
            for t in range(2):
                for i in range(height):
                    a = normalize(feat[0, t, pl.ds(c0, CHUNK), pl.ds(i * width, width)], c0)
                    u_buf[t, pl.ds(c0, CHUNK), pl.ds((i + 1) * width, width)] = a.astype(BF16)
            return 0

        lax.fori_loop(0, nchunk, norm_body, 0)
        for j in range(4):
            acc[j // 2, :, pl.ds((j % 2) * 128, 128)] = column(attn_b[j:j + 1, :])

        def bias(j):
            return jnp.concatenate([acc[j // 2, :, pl.ds((j % 2) * 128, 128)]] * height, axis=1)

        def frame(t, _):
            a = u_buf[t, pl.ds(0, channels), pl.ds(width, npos)]
            for j, ref in enumerate((attn_q, attn_k, attn_v)):
                ref[...] = (dot_t(attn_w[j], a) + bias(j)).astype(BF16)
            block = 256
            for qb in range(npos // block):
                cols = pl.ds(qb * block, block)
                s = dot_t(attn_k[...], attn_q[:, cols]) * channels ** -0.5
                p = jnp.exp(s - jnp.max(s, axis=0, keepdims=True))
                attn_p[:, cols] = (p * (1.0 / jnp.sum(p, axis=0, keepdims=True))).astype(BF16)
            attn_q[...] = jnp.dot(attn_v[...], attn_p[...], preferred_element_type=F32).astype(BF16)
            o = (dot_t(attn_w[3], attn_q[...]) + bias(3)).astype(BF16)
            feat[0, t] = (feat[0, t].astype(F32) + o.astype(F32)).astype(BF16)
            return 0

        lax.fori_loop(0, 2, frame, 0)

    x_copy().start()
    for a in (2, 1, 0):
        w_copy(0, a).start()
    barrier = pltpu.get_barrier_semaphore()
    for d in range(1, ranks):
        pl.semaphore_signal(barrier, inc=1, device_id={"time": lax.rem(me + d, ranks)}, device_id_type=MESH)
    for a in (2, 1, 0):
        w_copy(1, a).start()
    for s in range(4):
        for row in (0, height + 1):
            u_buf[s, :, pl.ds(row * width, width)] = jnp.zeros((k_tap, width), BF16)
    x_copy().wait()
    for t in range(2):
        feat[0, t] = x_in[t].T

    def plain_value(t, c0, i):
        return feat[0, t, pl.ds(c0, CHUNK), pl.ds(i * width, width)].astype(F32)

    accumulate_stats(plain_value)
    pl.semaphore_wait(barrier, ranks - 1)
    send_stats(0)
    start_halo(0)

    def conv_stage(k, _):
        src = k % 2
        dst = 1 - src
        n = k + k // 2
        slot = k % 2
        norm_coefs(n)
        for t in range(2):
            fill_u(frame_read(src, t), 2 + t)
        for a in (2, 1):
            w_copy(k, a).wait()
        acc[1] = dot_t(jnp.concatenate([w_buf[slot, 1], w_buf[slot, 2]], axis=0),
                       jnp.concatenate([taps(2), taps(3)], axis=0))
        acc[0] = dot_t(w_buf[slot, 2], taps(2))
        w_copy(k, 0).wait()
        get_halo(k, 1)
        acc[1] = acc[1] + dot_t(w_buf[slot, 0], taps(1))
        acc[0] = acc[0] + dot_t(w_buf[slot, 1], taps(1))
        get_halo(k, 0)
        acc[0] = acc[0] + dot_t(w_buf[slot, 0], taps(0))

        @pl.when(k < 2)
        def _():
            for a in (2, 1, 0):
                w_copy(k + 2, a).start()

        @pl.when(me < ranks - 1)
        def _():
            for t in (1, 0):
                halo_copy(k, t).wait_send()

        coef[0] = column(conv_b[pl.ds(k, 1), :])
        odd = src == 1

        def conv_value(t, c0, i):
            rows, cols = pl.ds(c0, CHUNK), pl.ds(i * width, width)
            h = (acc[t, rows, cols] + coef[0, rows, :]).astype(BF16).astype(F32)
            res = (feat[0, t, rows, cols].astype(F32) + h)
            y = jnp.where(odd, res, h).astype(BF16)
            feat[dst, t, rows, cols] = y
            return y.astype(F32)

        accumulate_stats(conv_value)

        @pl.when(k < 3)
        def _():
            send_stats(n + 1)

        @pl.when(src == 0)
        def _():
            start_halo(k + 1)

        @pl.when(k == 1)
        def _():
            norm_coefs(2)
            attention()
            accumulate_stats(plain_value)
            send_stats(3)
            start_halo(2)

        return 0

    lax.fori_loop(0, 4, conv_stage, 0)
    for t in range(2):
        out_ref[t] = feat[0, t].T


def solution(mesh):
    ranks = mesh.shape["time"]
    video_spec = P(("batch", "time"), None, None, None)

    def device_body(latent, conv_w, conv_b, norm_g, norm_b, attn_w, attn_b):
        frames, height, width, channels = latent.shape
        npos = height * width
        vmem = pl.BlockSpec(memory_space=pltpu.VMEM)
        hbm = pl.BlockSpec(memory_space=pl.ANY)
        dma = pltpu.SemaphoreType.DMA
        out = pl.pallas_call(
            functools.partial(kernel, ranks, height, width),
            out_shape=jax.ShapeDtypeStruct((frames, npos, channels), BF16),
            in_specs=[hbm, hbm] + [vmem] * 5,
            out_specs=vmem,
            scratch_shapes=[
                pltpu.VMEM((frames, npos, channels), BF16),
                pltpu.VMEM((2, 3, 9 * channels, channels), BF16),
                pltpu.VMEM((4, 3 * channels, (height + 2) * width), BF16),
                pltpu.VMEM((2, channels, npos), F32),
                pltpu.VMEM((2, 2, channels, npos), BF16),
                pltpu.VMEM((4, 2, channels, npos), BF16),
                pltpu.VMEM((2, channels, 128), F32),
                pltpu.VMEM((5, ranks, 2, channels), F32),
                pltpu.VMEM((3, channels, 128), F32),
                pltpu.VMEM((channels, npos), BF16),
                pltpu.VMEM((channels, npos), BF16),
                pltpu.VMEM((channels, npos), BF16),
                pltpu.VMEM((npos, npos), BF16),
                dma(()), dma((2, 3)), dma((5, ranks)), dma((5, ranks)), dma((4, 2)), dma((4, 2)),
            ],
            compiler_params=pltpu.CompilerParams(
                collective_id=0, has_side_effects=True, vmem_limit_bytes=62 * 2 ** 20),
            name="mid_block",
        )(latent.reshape(frames, npos, channels), conv_w.reshape(4, 3, 9 * channels, channels),
          conv_b, norm_g, norm_b, attn_w, attn_b)
        return out.reshape(latent.shape)

    return jax.shard_map(device_body, mesh=mesh, in_specs=(video_spec, P(), P(), P(), P(), P(), P()),
                         out_specs=video_spec, check_vma=False)
```

```python
import functools

import jax
import jax.numpy as jnp
from jax import lax
from jax.experimental import pallas as pl
from jax.experimental.pallas import tpu as pltpu
from jax.sharding import PartitionSpec as P

GROUPS = 32
NORM_EPS = 1e-6
CHUNK = 64
WIDE = 128
MESH = pl.DeviceIdType.MESH
F32 = jnp.float32
BF16 = jnp.bfloat16


def dot_t(lhs, rhs):
    return lax.dot_general(lhs, rhs, (((0,), (0,)), ((), ())), preferred_element_type=F32)


def kernel(ranks, height, width, x_hbm, w_hbm, conv_b, norm_g, norm_b, attn_w, attn_b, out_ref,
           x_in, w_buf, u_0, u_1, u_2, u_3, acc, feat, xres, halo, part, stat, coef, bias_col, member,
           attn_a, attn_q, attn_k, attn_v, attn_p,
           x_sem, w_sem, stat_send, stat_recv, halo_send, halo_recv):
    me = lax.axis_index("time")
    channels = feat.shape[3]
    u_bufs = (u_0, u_1, u_2, u_3)
    per_group = channels // GROUPS
    elem_count = float(ranks * 2 * height * width * per_group)
    npos = height * width
    nchunk = channels // CHUNK
    k_tap = 3 * channels

    def x_copy():
        return pltpu.make_async_copy(x_hbm, x_in, x_sem)

    def w_copy(k, a):
        return [pltpu.make_async_copy(w_hbm.at[k, a, :, pl.ds(j * 128, 128)], w_buf.at[k % 2, a, j],
                                      w_sem.at[k % 2, a, j]) for j in range(channels // 128)]

    def start_weights(k):
        for a in (2, 1, 0):
            for copy in w_copy(k, a):
                copy.start()

    def wait_weights(k, a):
        for copy in w_copy(k, a):
            copy.wait()

    def weights(slot, *taps_in_time):
        return jnp.concatenate([jnp.concatenate([w_buf[slot, a, j] for j in range(channels // 128)], axis=1)
                                for a in taps_in_time], axis=0)

    def wide(read):
        return jnp.concatenate([read(i) for i in range(height)], axis=1)

    def put(ref, value):
        for i in range(height):
            ref[i] = value[:, i * width:(i + 1) * width]

    def stat_copy(n, source, target):
        return pltpu.make_async_remote_copy(
            src_ref=stat.at[n, source], dst_ref=stat.at[n, source], send_sem=stat_send.at[n, target],
            recv_sem=stat_recv.at[n, source], device_id={"time": target}, device_id_type=MESH)

    def halo_copy(k, t):
        return pltpu.make_async_remote_copy(
            src_ref=feat.at[k % 2, t], dst_ref=halo.at[k, t], send_sem=halo_send.at[k, t],
            recv_sem=halo_recv.at[k, t], device_id={"time": lax.rem(me + 1, ranks)}, device_id_type=MESH)

    def start_halo(k):
        @pl.when(me < ranks - 1)
        def _():
            for t in (1, 0):
                halo_copy(k, t).start()

    def send_stats(n):
        rows = [jnp.sum(part[i].T, axis=0, keepdims=True) for i in range(2)]
        stat[n, me] = jnp.concatenate(rows, axis=0)
        for d in range(1, ranks):
            stat_copy(n, me, lax.rem(me + d, ranks)).start()

    def column(row):
        return jnp.broadcast_to(row, (128, channels)).T

    def norm_coefs(n):
        coef[2] = column(norm_b[pl.ds(n, 1), :])
        for d in range(1, ranks):
            stat_copy(n, lax.rem(me + d, ranks), lax.rem(me + d, ranks)).wait_recv()
        totals = jnp.sum(stat[n], axis=0)
        totals = jnp.concatenate([totals, jnp.zeros((6, channels), F32)], axis=0)
        high = totals.astype(BF16).astype(F32)
        rest = totals - high
        mid = rest.astype(BF16).astype(F32)
        low = rest - mid
        parts = jnp.concatenate([high, mid, low, jnp.zeros_like(low)], axis=0).astype(BF16)
        sums = jnp.dot(parts, member[...], preferred_element_type=F32)
        sums = sums[0:8] + sums[8:16] + sums[16:24]
        mean = sums[0:1] / elem_count
        var = sums[1:2] / elem_count - mean * mean
        scale = lax.rsqrt(var + NORM_EPS) * norm_g[pl.ds(n, 1), :]
        coef[0] = column(mean)
        coef[1] = column(scale)
        for d in range(1, ranks):
            stat_copy(n, me, lax.rem(me + d, ranks)).wait_send()

    def normalize(value, c0, size=CHUNK):
        sl = pl.ds(c0, size)
        return (value.astype(F32) - coef[0, sl, :]) * coef[1, sl, :] + coef[2, sl, :]

    def fill_rows(read, s, c0, size):
        lane = lax.broadcasted_iota(jnp.int32, (size, width), 1)
        for i in range(height):
            half = 0.5 * normalize(read(c0, size, i), c0, size)
            u = (half + half * jnp.tanh(half)).astype(BF16)
            left = jnp.where(lane == 0, jnp.zeros_like(u), pltpu.roll(u, 1, 1))
            right = jnp.where(lane == width - 1, jnp.zeros_like(u), pltpu.roll(u, width - 1, 1))
            for e, v in enumerate((left, u, right)):
                u_bufs[s][i + 1, pl.ds(e * channels + c0, size), :] = v

    def fill_u(read, s):
        def body(ci, _):
            fill_rows(read, s, pl.multiple_of(ci * WIDE, WIDE), WIDE)
            return 0

        lax.fori_loop(0, channels // WIDE, body, 0)

    def taps(s):
        return jnp.concatenate([wide(lambda i: u_bufs[s][d + i]) for d in range(3)], axis=0)

    def frame_read(b, t):
        return lambda c0, size, i: feat[b, t, i, pl.ds(c0, size), :]

    def halo_read(k, t):
        return lambda c0, size, i: halo[k, t, i, pl.ds(c0, size), :]

    def get_halo(k, t):
        @pl.when(me > 0)
        def _():
            halo_copy(k, t).wait_recv()

        @pl.when(me == 0)
        def _():
            halo[k, t] = feat[k % 2, 0]

        fill_u(halo_read(k, t), t)

    def accumulate_stats(value_of):
        def body(ci, _):
            c0 = pl.multiple_of(ci * CHUNK, CHUNK)
            s1 = jnp.zeros((CHUNK, width), F32)
            s2 = jnp.zeros((CHUNK, width), F32)
            for t in range(2):
                for i in range(height):
                    v = value_of(t, c0, i)
                    s1 = s1 + v
                    s2 = s2 + v * v
            part[0, pl.ds(c0, CHUNK), :] = s1
            part[1, pl.ds(c0, CHUNK), :] = s2
            return 0

        lax.fori_loop(0, nchunk, body, 0)

    def attention():
        def norm_body(ci, _):
            c0 = pl.multiple_of(ci * CHUNK, CHUNK)
            for t in range(2):
                for i in range(height):
                    a = normalize(feat[0, t, i, pl.ds(c0, CHUNK), :], c0)
                    attn_a[t, i, pl.ds(c0, CHUNK), :] = a.astype(BF16)
            return 0

        lax.fori_loop(0, nchunk, norm_body, 0)
        for j in range(4):
            acc[0, j] = column(attn_b[j:j + 1, :])

        def bias(j):
            return jnp.concatenate([acc[0, j]] * height, axis=1)

        def frame(t, _):
            a = wide(lambda i: attn_a[t, i])
            for j, ref in enumerate((attn_q, attn_k, attn_v)):
                put(ref, (dot_t(attn_w[j], a) + bias(j)).astype(BF16))
            keys = wide(lambda i: attn_k[i])
            for qb in range(height // 2):
                query = jnp.concatenate([attn_q[2 * qb], attn_q[2 * qb + 1]], axis=1)
                s = dot_t(keys, query) * channels ** -0.5
                p = jnp.exp(s - jnp.max(s, axis=0, keepdims=True))
                p = (p * (1.0 / jnp.sum(p, axis=0, keepdims=True))).astype(BF16)
                attn_p[2 * qb] = p[:, :width]
                attn_p[2 * qb + 1] = p[:, width:]
            mixed = jnp.dot(wide(lambda i: attn_v[i]), wide(lambda i: attn_p[i]), preferred_element_type=F32)
            put(attn_q, mixed.astype(BF16))
            o = (dot_t(attn_w[3], wide(lambda i: attn_q[i])) + bias(3)).astype(BF16).astype(F32)
            for i in range(height):
                y = (feat[0, t, i].astype(F32) + o[:, i * width:(i + 1) * width]).astype(BF16)
                feat[0, t, i] = y
                xres[t, i] = y
            return 0

        lax.fori_loop(0, 2, frame, 0)

    x_copy().start()
    start_weights(0)
    barrier = pltpu.get_barrier_semaphore()
    for d in range(1, ranks):
        pl.semaphore_signal(barrier, inc=1, device_id={"time": lax.rem(me + d, ranks)}, device_id_type=MESH)
    start_weights(1)
    for s in range(4):
        for row in (0, height + 1):
            u_bufs[s][row] = jnp.zeros((k_tap, width), BF16)
    magic = (65536 + per_group - 1) // per_group
    r = lax.broadcasted_iota(jnp.int32, (channels, channels), 0) * magic // 65536
    c = lax.broadcasted_iota(jnp.int32, (channels, channels), 1) * magic // 65536
    member[...] = jnp.where(r == c, 1.0, 0.0).astype(BF16)
    x_copy().wait()
    for t in range(2):
        for i in range(height):
            x = x_in[t, pl.ds(i * width, width), :].T
            feat[0, t, i] = x
            xres[t, i] = x

    def plain_value(t, c0, i):
        return feat[0, t, i, pl.ds(c0, CHUNK), :].astype(F32)

    accumulate_stats(plain_value)
    pl.semaphore_wait(barrier, ranks - 1)
    send_stats(0)
    start_halo(0)

    def conv_stage(k, _):
        src = k % 2
        dst = 1 - src
        n = k + k // 2
        slot = k % 2
        bias_col[...] = column(conv_b[pl.ds(k, 1), :])
        norm_coefs(n)
        fill_u(frame_read(src, 0), 2)
        wait_weights(k, 2)
        wait_weights(k, 1)
        put(acc.at[0], dot_t(weights(slot, 2), taps(2)))
        for c0 in range(0, channels, CHUNK):
            fill_rows(frame_read(src, 1), 3, c0, CHUNK)
        put(acc.at[1], dot_t(weights(slot, 1, 2), jnp.concatenate([taps(2), taps(3)], axis=0)))
        wait_weights(k, 0)
        get_halo(k, 1)
        put(acc.at[1], wide(lambda i: acc[1, i]) + dot_t(weights(slot, 0), taps(1)))
        put(acc.at[0], wide(lambda i: acc[0, i]) + dot_t(weights(slot, 1), taps(1)))
        get_halo(k, 0)

        @pl.when(me < ranks - 1)
        def _():
            for t in (1, 0):
                halo_copy(k, t).wait_send()

        odd = src == 1

        def finish(t, value):
            for c0 in range(0, channels, CHUNK):
                rows = pl.ds(c0, CHUNK)
                s1 = jnp.zeros((CHUNK, width), F32) if t else part[0, rows, :]
                s2 = jnp.zeros((CHUNK, width), F32) if t else part[1, rows, :]
                ys = []
                for i in range(height):
                    h = (value(i, c0) + bias_col[rows, :]).astype(BF16).astype(F32)
                    y = jnp.where(odd, xres[t, i, rows, :].astype(F32) + h, h).astype(BF16)
                    ys.append(y)
                    y = y.astype(F32)
                    s1 = s1 + y
                    s2 = s2 + y * y
                for i in range(height):
                    feat[dst, t, i, rows, :] = ys[i]
                part[0, rows, :] = s1
                part[1, rows, :] = s2

        last = dot_t(weights(slot, 0), taps(0))
        finish(1, lambda i, c0: acc[1, i, pl.ds(c0, CHUNK), :])
        finish(0, lambda i, c0: acc[0, i, pl.ds(c0, CHUNK), :]
               + last[c0:c0 + CHUNK, i * width:(i + 1) * width])

        @pl.when(k < 2)
        def _():
            start_weights(k + 2)

        @pl.when(k < 3)
        def _():
            send_stats(n + 1)

        @pl.when(src == 0)
        def _():
            start_halo(k + 1)

        @pl.when(k == 1)
        def _():
            norm_coefs(2)
            attention()
            accumulate_stats(plain_value)
            send_stats(3)
            start_halo(2)

        return 0

    lax.fori_loop(0, 4, conv_stage, 0)
    for t in range(2):
        for i in range(height):
            out_ref[t, pl.ds(i * width, width), :] = feat[0, t, i].T


def solution(mesh):
    ranks = mesh.shape["time"]
    video_spec = P(("batch", "time"), None, None, None)

    def device_body(latent, conv_w, conv_b, norm_g, norm_b, attn_w, attn_b):
        frames, height, width, channels = latent.shape
        npos = height * width
        vmem = pl.BlockSpec(memory_space=pltpu.VMEM)
        hbm = pl.BlockSpec(memory_space=pl.ANY)
        dma = pltpu.SemaphoreType.DMA
        out = pl.pallas_call(
            functools.partial(kernel, ranks, height, width),
            out_shape=jax.ShapeDtypeStruct((frames, npos, channels), BF16),
            in_specs=[hbm, hbm] + [vmem] * 5,
            out_specs=vmem,
            scratch_shapes=[
                pltpu.VMEM((frames, npos, channels), BF16),
                pltpu.VMEM((2, 3, channels // 128, 9 * channels, 128), BF16),
                pltpu.VMEM((height + 2, 3 * channels, width), BF16),
                pltpu.VMEM((height + 2, 3 * channels, width), BF16),
                pltpu.VMEM((height + 2, 3 * channels, width), BF16),
                pltpu.VMEM((height + 2, 3 * channels, width), BF16),
                pltpu.VMEM((2, height, channels, width), F32),
                pltpu.VMEM((2, 2, height, channels, width), BF16),
                pltpu.VMEM((2, height, channels, width), BF16),
                pltpu.VMEM((4, 2, height, channels, width), BF16),
                pltpu.VMEM((2, channels, 128), F32),
                pltpu.VMEM((5, ranks, 2, channels), F32),
                pltpu.VMEM((3, channels, 128), F32),
                pltpu.VMEM((channels, 128), F32),
                pltpu.VMEM((channels, channels), BF16),
                pltpu.VMEM((2, height, channels, width), BF16),
                pltpu.VMEM((height, channels, width), BF16),
                pltpu.VMEM((height, channels, width), BF16),
                pltpu.VMEM((height, channels, width), BF16),
                pltpu.VMEM((height, npos, width), BF16),
                dma(()), dma((2, 3, channels // 128)), dma((5, ranks)), dma((5, ranks)), dma((4, 2)), dma((4, 2)),
            ],
            compiler_params=pltpu.CompilerParams(
                collective_id=0, has_side_effects=True, vmem_limit_bytes=62 * 2 ** 20),
            name="mid_block",
        )(latent.reshape(frames, npos, channels), conv_w.reshape(4, 3, 9 * channels, channels),
          conv_b, norm_g, norm_b, attn_w, attn_b)
        return out.reshape(latent.shape)

    return jax.shard_map(device_body, mesh=mesh, in_specs=(video_spec, P(), P(), P(), P(), P(), P()),
                         out_specs=video_spec, check_vma=False)
```

```python
import functools

import jax
import jax.numpy as jnp
from jax import lax
from jax.experimental import pallas as pl
from jax.experimental.pallas import tpu as pltpu
from jax.sharding import PartitionSpec as P

GROUPS = 32
NORM_EPS = 1e-6
CHUNK = 64
MESH = pl.DeviceIdType.MESH
F32 = jnp.float32
BF16 = jnp.bfloat16


def dot_t(lhs, rhs):
    return lax.dot_general(lhs, rhs, (((0,), (0,)), ((), ())), preferred_element_type=F32)


def kernel(ranks, height, width, x_hbm, w_hbm, conv_b, norm_g, norm_b, attn_w, attn_b, out_ref,
           x_in, w_buf, u_0, u_1, u_2, u_3, acc, feat, xres, halo, part, stat, coef, bias_col, member,
           attn_a, attn_q, attn_k, attn_v, attn_p,
           x_sem, w_sem, stat_send, stat_recv, halo_send, halo_recv):
    me = lax.axis_index("time")
    channels = feat.shape[3]
    u_bufs = (u_0, u_1, u_2, u_3)
    per_group = channels // GROUPS
    elem_count = float(ranks * 2 * height * width * per_group)
    npos = height * width
    nchunk = channels // CHUNK
    k_tap = 3 * channels

    def x_copy():
        return pltpu.make_async_copy(x_hbm, x_in, x_sem)

    def w_copy(k, a):
        return [pltpu.make_async_copy(w_hbm.at[k, a, :, pl.ds(j * 128, 128)], w_buf.at[k % 2, a, j],
                                      w_sem.at[k % 2, a, j]) for j in range(channels // 128)]

    def start_weights(k):
        for a in (2, 1, 0):
            for copy in w_copy(k, a):
                copy.start()

    def wait_weights(k, a):
        for copy in w_copy(k, a):
            copy.wait()

    def weights(slot, *taps_in_time):
        return jnp.concatenate([jnp.concatenate([w_buf[slot, a, j] for j in range(channels // 128)], axis=1)
                                for a in taps_in_time], axis=0)

    def wide(read):
        return jnp.concatenate([read(i) for i in range(height)], axis=1)

    def put(ref, value):
        for i in range(height):
            ref[i] = value[:, i * width:(i + 1) * width]

    def stat_copy(n, source, target):
        return pltpu.make_async_remote_copy(
            src_ref=stat.at[n, source], dst_ref=stat.at[n, source], send_sem=stat_send.at[n, target],
            recv_sem=stat_recv.at[n, source], device_id={"time": target}, device_id_type=MESH)

    def halo_copy(k, t):
        return pltpu.make_async_remote_copy(
            src_ref=feat.at[k % 2, t], dst_ref=halo.at[k, t], send_sem=halo_send.at[k, t],
            recv_sem=halo_recv.at[k, t], device_id={"time": lax.rem(me + 1, ranks)}, device_id_type=MESH)

    def start_halo(k):
        @pl.when(me < ranks - 1)
        def _():
            for t in (1, 0):
                halo_copy(k, t).start()

    def send_stats(n):
        rows = [jnp.sum(part[i].T, axis=0, keepdims=True) for i in range(2)]
        stat[n, me] = jnp.concatenate(rows, axis=0)
        for d in sorted(range(1, ranks), key=lambda d: -min(d, ranks - d)):
            stat_copy(n, me, lax.rem(me + d, ranks)).start()

    def column(row):
        return jnp.broadcast_to(row, (128, channels)).T

    def norm_coefs(n, factor):
        coef[2] = column(norm_b[pl.ds(n, 1), :] * factor)
        for d in range(1, ranks):
            stat_copy(n, lax.rem(me + d, ranks), lax.rem(me + d, ranks)).wait_recv()
        totals = jnp.sum(stat[n], axis=0)
        totals = jnp.concatenate([totals, jnp.zeros((6, channels), F32)], axis=0)
        high = totals.astype(BF16).astype(F32)
        rest = totals - high
        mid = rest.astype(BF16).astype(F32)
        low = rest - mid
        parts = jnp.concatenate([high, mid, low, jnp.zeros_like(low)], axis=0).astype(BF16)
        sums = jnp.dot(parts, member[...], preferred_element_type=F32)
        sums = sums[0:8] + sums[8:16] + sums[16:24]
        mean = sums[0:1] / elem_count
        var = sums[1:2] / elem_count - mean * mean
        scale = lax.rsqrt(var + NORM_EPS) * norm_g[pl.ds(n, 1), :] * factor
        coef[0] = column(mean)
        coef[1] = column(scale)
        for d in range(1, ranks):
            stat_copy(n, me, lax.rem(me + d, ranks)).wait_send()

    def normalize(value, c0, size=CHUNK):
        sl = pl.ds(c0, size)
        return (value.astype(F32) - coef[0, sl, :]) * coef[1, sl, :] + coef[2, sl, :]

    def fill_rows(read, s, c0, size):
        lane = lax.broadcasted_iota(jnp.int32, (size, width), 1)
        for i in range(height):
            half = normalize(read(c0, size, i), c0, size)
            u = (half + half * jnp.tanh(half)).astype(BF16)
            left = jnp.where(lane == 0, jnp.zeros_like(u), pltpu.roll(u, 1, 1))
            right = jnp.where(lane == width - 1, jnp.zeros_like(u), pltpu.roll(u, width - 1, 1))
            for e, v in enumerate((left, u, right)):
                u_bufs[s][i + 1, pl.ds(e * channels + c0, size), :] = v

    def fill_u(read, s):
        @pl.when(me >= 0)
        def _():
            for c0 in range(0, channels, CHUNK):
                fill_rows(read, s, c0, CHUNK)

    def taps(s):
        return jnp.concatenate([wide(lambda i: u_bufs[s][d + i]) for d in range(3)], axis=0)

    def frame_read(b, t):
        return lambda c0, size, i: feat[b, t, i, pl.ds(c0, size), :]

    def halo_read(k, t):
        return lambda c0, size, i: halo[k, t, i, pl.ds(c0, size), :]

    def get_halo(k, t):
        @pl.when(me > 0)
        def _():
            halo_copy(k, t).wait_recv()

        @pl.when(me == 0)
        def _():
            halo[k, t] = feat[k % 2, 0]

        fill_u(halo_read(k, t), t)

    def accumulate_stats(value_of):
        def body(ci, _):
            c0 = pl.multiple_of(ci * CHUNK, CHUNK)
            s1 = jnp.zeros((CHUNK, width), F32)
            s2 = jnp.zeros((CHUNK, width), F32)
            for t in range(2):
                for i in range(height):
                    v = value_of(t, c0, i)
                    s1 = s1 + v
                    s2 = s2 + v * v
            part[0, pl.ds(c0, CHUNK), :] = s1
            part[1, pl.ds(c0, CHUNK), :] = s2
            return 0

        lax.fori_loop(0, nchunk, body, 0)

    def attention():
        def norm_body(ci, _):
            c0 = pl.multiple_of(ci * CHUNK, CHUNK)
            for t in range(2):
                for i in range(height):
                    a = normalize(feat[0, t, i, pl.ds(c0, CHUNK), :], c0)
                    attn_a[t, i, pl.ds(c0, CHUNK), :] = a.astype(BF16)
            return 0

        lax.fori_loop(0, nchunk, norm_body, 0)
        for j in range(4):
            acc[0, j] = column(attn_b[j:j + 1, :])

        def bias(j):
            return jnp.concatenate([acc[0, j]] * height, axis=1)

        def frame(t, _):
            a = wide(lambda i: attn_a[t, i])
            for j, ref in enumerate((attn_q, attn_k, attn_v)):
                put(ref, (dot_t(attn_w[j], a) + bias(j)).astype(BF16))
            keys = wide(lambda i: attn_k[i])
            for qb in range(height // 2):
                query = jnp.concatenate([attn_q[2 * qb], attn_q[2 * qb + 1]], axis=1)
                s = dot_t(keys, query) * channels ** -0.5
                p = jnp.exp(s - jnp.max(s, axis=0, keepdims=True))
                p = (p * (1.0 / jnp.sum(p, axis=0, keepdims=True))).astype(BF16)
                attn_p[2 * qb] = p[:, :width]
                attn_p[2 * qb + 1] = p[:, width:]
            mixed = jnp.dot(wide(lambda i: attn_v[i]), wide(lambda i: attn_p[i]), preferred_element_type=F32)
            put(attn_q, mixed.astype(BF16))
            o = (dot_t(attn_w[3], wide(lambda i: attn_q[i])) + bias(3)).astype(BF16).astype(F32)
            for i in range(height):
                y = (feat[0, t, i].astype(F32) + o[:, i * width:(i + 1) * width]).astype(BF16)
                feat[0, t, i] = y
                xres[t, i] = y
            return 0

        lax.fori_loop(0, 2, frame, 0)

    x_copy().start()
    start_weights(0)
    barrier = pltpu.get_barrier_semaphore()
    for d in range(1, ranks):
        pl.semaphore_signal(barrier, inc=1, device_id={"time": lax.rem(me + d, ranks)}, device_id_type=MESH)
    start_weights(1)
    for s in range(4):
        for row in (0, height + 1):
            u_bufs[s][row] = jnp.zeros((k_tap, width), BF16)
    magic = (65536 + per_group - 1) // per_group
    r = lax.broadcasted_iota(jnp.int32, (channels, channels), 0) * magic // 65536
    c = lax.broadcasted_iota(jnp.int32, (channels, channels), 1) * magic // 65536
    member[...] = jnp.where(r == c, 1.0, 0.0).astype(BF16)
    x_copy().wait()
    for t in range(2):
        for i in range(height):
            x = x_in[t, pl.ds(i * width, width), :].T
            feat[0, t, i] = x
            xres[t, i] = x

    def plain_value(t, c0, i):
        return feat[0, t, i, pl.ds(c0, CHUNK), :].astype(F32)

    accumulate_stats(plain_value)
    pl.semaphore_wait(barrier, ranks - 1)
    send_stats(0)
    start_halo(0)

    def conv_stage(k, _):
        src = k % 2
        dst = 1 - src
        n = k + k // 2
        slot = k % 2
        bias_col[...] = column(conv_b[pl.ds(k, 1), :])
        norm_coefs(n, 0.5)
        fill_u(frame_read(src, 0), 2)
        wait_weights(k, 2)
        wait_weights(k, 1)
        put(acc.at[0], dot_t(weights(slot, 2), taps(2)))
        for c0 in range(0, channels, CHUNK):
            fill_rows(frame_read(src, 1), 3, c0, CHUNK)
        put(acc.at[1], dot_t(weights(slot, 1, 2), jnp.concatenate([taps(2), taps(3)], axis=0)))
        wait_weights(k, 0)
        get_halo(k, 1)
        put(acc.at[1], wide(lambda i: acc[1, i]) + dot_t(weights(slot, 0), taps(1)))
        put(acc.at[0], wide(lambda i: acc[0, i]) + dot_t(weights(slot, 1), taps(1)))
        get_halo(k, 0)

        @pl.when(me < ranks - 1)
        def _():
            for t in (1, 0):
                halo_copy(k, t).wait_send()

        odd = src == 1

        def finish(t, value):
            for c0 in range(0, channels, CHUNK):
                rows = pl.ds(c0, CHUNK)
                s1 = jnp.zeros((CHUNK, width), F32) if t else part[0, rows, :]
                s2 = jnp.zeros((CHUNK, width), F32) if t else part[1, rows, :]
                ys = []
                for i in range(height):
                    h = (value(i, c0) + bias_col[rows, :]).astype(BF16).astype(F32)
                    y = jnp.where(odd, xres[t, i, rows, :].astype(F32) + h, h).astype(BF16)
                    ys.append(y)
                    y = y.astype(F32)
                    s1 = s1 + y
                    s2 = s2 + y * y
                for i in range(height):
                    feat[dst, t, i, rows, :] = ys[i]
                part[0, rows, :] = s1
                part[1, rows, :] = s2

        last = dot_t(weights(slot, 0), taps(0))
        finish(1, lambda i, c0: acc[1, i, pl.ds(c0, CHUNK), :])
        finish(0, lambda i, c0: acc[0, i, pl.ds(c0, CHUNK), :]
               + last[c0:c0 + CHUNK, i * width:(i + 1) * width])

        @pl.when(k < 2)
        def _():
            start_weights(k + 2)

        @pl.when(k < 3)
        def _():
            send_stats(n + 1)

        @pl.when(src == 0)
        def _():
            start_halo(k + 1)

        @pl.when(k == 1)
        def _():
            norm_coefs(2, 1.0)
            attention()
            accumulate_stats(plain_value)
            send_stats(3)
            start_halo(2)

        return 0

    lax.fori_loop(0, 4, conv_stage, 0)
    for t in range(2):
        for i in range(height):
            out_ref[t, pl.ds(i * width, width), :] = feat[0, t, i].T


def solution(mesh):
    ranks = mesh.shape["time"]
    video_spec = P(("batch", "time"), None, None, None)

    def device_body(latent, conv_w, conv_b, norm_g, norm_b, attn_w, attn_b):
        frames, height, width, channels = latent.shape
        npos = height * width
        vmem = pl.BlockSpec(memory_space=pltpu.VMEM)
        hbm = pl.BlockSpec(memory_space=pl.ANY)
        dma = pltpu.SemaphoreType.DMA
        out = pl.pallas_call(
            functools.partial(kernel, ranks, height, width),
            out_shape=jax.ShapeDtypeStruct((frames, npos, channels), BF16),
            in_specs=[hbm, hbm] + [vmem] * 5,
            out_specs=vmem,
            scratch_shapes=[
                pltpu.VMEM((frames, npos, channels), BF16),
                pltpu.VMEM((2, 3, channels // 128, 9 * channels, 128), BF16),
                pltpu.VMEM((height + 2, 3 * channels, width), BF16),
                pltpu.VMEM((height + 2, 3 * channels, width), BF16),
                pltpu.VMEM((height + 2, 3 * channels, width), BF16),
                pltpu.VMEM((height + 2, 3 * channels, width), BF16),
                pltpu.VMEM((2, height, channels, width), F32),
                pltpu.VMEM((2, 2, height, channels, width), BF16),
                pltpu.VMEM((2, height, channels, width), BF16),
                pltpu.VMEM((4, 2, height, channels, width), BF16),
                pltpu.VMEM((2, channels, 128), F32),
                pltpu.VMEM((5, ranks, 2, channels), F32),
                pltpu.VMEM((3, channels, 128), F32),
                pltpu.VMEM((channels, 128), F32),
                pltpu.VMEM((channels, channels), BF16),
                pltpu.VMEM((2, height, channels, width), BF16),
                pltpu.VMEM((height, channels, width), BF16),
                pltpu.VMEM((height, channels, width), BF16),
                pltpu.VMEM((height, channels, width), BF16),
                pltpu.VMEM((height, npos, width), BF16),
                dma(()), dma((2, 3, channels // 128)), dma((5, ranks)), dma((5, ranks)), dma((4, 2)), dma((4, 2)),
            ],
            compiler_params=pltpu.CompilerParams(
                collective_id=0, has_side_effects=True, vmem_limit_bytes=62 * 2 ** 20),
            name="mid_block",
        )(latent.reshape(frames, npos, channels), conv_w.reshape(4, 3, 9 * channels, channels),
          conv_b, norm_g, norm_b, attn_w, attn_b)
        return out.reshape(latent.shape)

    return jax.shard_map(device_body, mesh=mesh, in_specs=(video_spec, P(), P(), P(), P(), P(), P()),
                         out_specs=video_spec, check_vma=False)
```

```python
import functools

import jax
import jax.numpy as jnp
from jax import lax
from jax.experimental import pallas as pl
from jax.experimental.pallas import tpu as pltpu
from jax.sharding import PartitionSpec as P

GROUPS = 32
NORM_EPS = 1e-6
CHUNK = 64
MESH = pl.DeviceIdType.MESH
F32 = jnp.float32
BF16 = jnp.bfloat16


def dot_t(lhs, rhs):
    return lax.dot_general(lhs, rhs, (((0,), (0,)), ((), ())), preferred_element_type=F32)


def kernel(ranks, height, width, x_hbm, w_hbm, conv_b_hbm, norm_g_hbm, norm_b_hbm, attn_w_hbm, attn_b_hbm, out_hbm,
           conv_b, norm_g, norm_b, attn_w, attn_b,
           x_in, w_buf, u_0, u_1, u_2, u_3, acc, feat, xres, halo, part, stat, coef, bias_col, member,
           attn_a, attn_q, attn_k, attn_v, attn_p,
           x_sem, param_sem, out_sem, w_sem, stat_send, stat_recv, halo_send, halo_recv):
    me = lax.axis_index("time")
    channels = feat.shape[3]
    u_bufs = (u_0, u_1, u_2, u_3)
    per_group = channels // GROUPS
    elem_count = float(ranks * 2 * height * width * per_group)
    npos = height * width
    nchunk = channels // CHUNK
    k_tap = 3 * channels

    def x_copy():
        return pltpu.make_async_copy(x_hbm, x_in, x_sem)

    def w_copy(k, a):
        return [pltpu.make_async_copy(w_hbm.at[k, a, :, pl.ds(j * 128, 128)], w_buf.at[k % 2, a, j],
                                      w_sem.at[k % 2, a, j]) for j in range(channels // 128)]

    def start_weights(k):
        for a in (2, 1, 0):
            for copy in w_copy(k, a):
                copy.start()

    def wait_weights(k, a):
        for copy in w_copy(k, a):
            copy.wait()

    def weights(slot, *taps_in_time):
        return jnp.concatenate([jnp.concatenate([w_buf[slot, a, j] for j in range(channels // 128)], axis=1)
                                for a in taps_in_time], axis=0)

    def wide(read):
        return jnp.concatenate([read(i) for i in range(height)], axis=1)

    def put(ref, value):
        for i in range(height):
            ref[i] = value[:, i * width:(i + 1) * width]

    params = ((conv_b_hbm, conv_b), (norm_g_hbm, norm_g), (norm_b_hbm, norm_b), (attn_b_hbm, attn_b),
              (attn_w_hbm, attn_w))

    def param_copy(j):
        return pltpu.make_async_copy(params[j][0], params[j][1], param_sem.at[j])

    def stat_copy(n, source, target):
        return pltpu.make_async_remote_copy(
            src_ref=stat.at[n, source], dst_ref=stat.at[n, source], send_sem=stat_send.at[n, target],
            recv_sem=stat_recv.at[n, source], device_id={"time": target}, device_id_type=MESH)

    def halo_copy(k, t):
        return pltpu.make_async_remote_copy(
            src_ref=feat.at[k % 2, t], dst_ref=halo.at[k, t], send_sem=halo_send.at[k, t],
            recv_sem=halo_recv.at[k, t], device_id={"time": lax.rem(me + 1, ranks)}, device_id_type=MESH)

    def start_halo(k):
        @pl.when(me < ranks - 1)
        def _():
            for t in (1, 0):
                halo_copy(k, t).start()

    def send_stats(n):
        rows = [jnp.sum(part[i].T, axis=0, keepdims=True) for i in range(2)]
        stat[n, me] = jnp.concatenate(rows, axis=0)
        for d in sorted(range(1, ranks), key=lambda d: -min(d, ranks - d)):
            stat_copy(n, me, lax.rem(me + d, ranks)).start()

    def column(row):
        return jnp.broadcast_to(row, (128, channels)).T

    def norm_coefs(n, factor):
        coef[2] = column(norm_b[pl.ds(n, 1), :] * factor)
        for d in range(1, ranks):
            stat_copy(n, lax.rem(me + d, ranks), lax.rem(me + d, ranks)).wait_recv()
        totals = jnp.sum(stat[n], axis=0)
        totals = jnp.concatenate([totals, jnp.zeros((6, channels), F32)], axis=0)
        high = totals.astype(BF16).astype(F32)
        rest = totals - high
        mid = rest.astype(BF16).astype(F32)
        low = rest - mid
        parts = jnp.concatenate([high, mid, low, jnp.zeros_like(low)], axis=0).astype(BF16)
        sums = jnp.dot(parts, member[...], preferred_element_type=F32)
        sums = sums[0:8] + sums[8:16] + sums[16:24]
        mean = sums[0:1] / elem_count
        var = sums[1:2] / elem_count - mean * mean
        scale = lax.rsqrt(var + NORM_EPS) * norm_g[pl.ds(n, 1), :] * factor
        coef[0] = column(mean)
        coef[1] = column(scale)
        for d in range(1, ranks):
            stat_copy(n, me, lax.rem(me + d, ranks)).wait_send()

    def normalize(value, c0, size=CHUNK):
        sl = pl.ds(c0, size)
        return (value.astype(F32) - coef[0, sl, :]) * coef[1, sl, :] + coef[2, sl, :]

    def fill_rows(read, s, c0, size):
        lane = lax.broadcasted_iota(jnp.int32, (size, width), 1)
        for i in range(height):
            half = normalize(read(c0, size, i), c0, size)
            u = (half + half * jnp.tanh(half)).astype(BF16)
            left = jnp.where(lane == 0, jnp.zeros_like(u), pltpu.roll(u, 1, 1))
            right = jnp.where(lane == width - 1, jnp.zeros_like(u), pltpu.roll(u, width - 1, 1))
            for e, v in enumerate((left, u, right)):
                u_bufs[s][i + 1, pl.ds(e * channels + c0, size), :] = v

    def fill_u(read, s):
        @pl.when(me >= 0)
        def _():
            for c0 in range(0, channels, CHUNK):
                fill_rows(read, s, c0, CHUNK)

    def taps(s):
        return jnp.concatenate([wide(lambda i: u_bufs[s][d + i]) for d in range(3)], axis=0)

    def frame_read(b, t):
        return lambda c0, size, i: feat[b, t, i, pl.ds(c0, size), :]

    def halo_read(k, t):
        return lambda c0, size, i: halo[k, t, i, pl.ds(c0, size), :]

    def get_halo(k, t):
        @pl.when(me > 0)
        def _():
            halo_copy(k, t).wait_recv()

        @pl.when(me == 0)
        def _():
            halo[k, t] = feat[k % 2, 0]

        fill_u(halo_read(k, t), t)

    def accumulate_stats(value_of):
        def body(ci, _):
            c0 = pl.multiple_of(ci * CHUNK, CHUNK)
            s1 = jnp.zeros((CHUNK, width), F32)
            s2 = jnp.zeros((CHUNK, width), F32)
            for t in range(2):
                for i in range(height):
                    v = value_of(t, c0, i)
                    s1 = s1 + v
                    s2 = s2 + v * v
            part[0, pl.ds(c0, CHUNK), :] = s1
            part[1, pl.ds(c0, CHUNK), :] = s2
            return 0

        lax.fori_loop(0, nchunk, body, 0)

    def attention():
        def norm_body(ci, _):
            c0 = pl.multiple_of(ci * CHUNK, CHUNK)
            for t in range(2):
                for i in range(height):
                    a = normalize(feat[0, t, i, pl.ds(c0, CHUNK), :], c0)
                    attn_a[t, i, pl.ds(c0, CHUNK), :] = a.astype(BF16)
            return 0

        lax.fori_loop(0, nchunk, norm_body, 0)
        for j in range(4):
            acc[0, j] = column(attn_b[j:j + 1, :])

        def bias(j):
            return jnp.concatenate([acc[0, j]] * height, axis=1)

        def frame(t, _):
            a = wide(lambda i: attn_a[t, i])
            for j, ref in enumerate((attn_q, attn_k, attn_v)):
                put(ref, (dot_t(attn_w[j], a) + bias(j)).astype(BF16))
            keys = wide(lambda i: attn_k[i])
            for qb in range(height // 2):
                query = jnp.concatenate([attn_q[2 * qb], attn_q[2 * qb + 1]], axis=1)
                s = dot_t(keys, query) * channels ** -0.5
                p = jnp.exp(s - jnp.max(s, axis=0, keepdims=True))
                p = (p * (1.0 / jnp.sum(p, axis=0, keepdims=True))).astype(BF16)
                attn_p[2 * qb] = p[:, :width]
                attn_p[2 * qb + 1] = p[:, width:]
            mixed = jnp.dot(wide(lambda i: attn_v[i]), wide(lambda i: attn_p[i]), preferred_element_type=F32)
            put(attn_q, mixed.astype(BF16))
            o = (dot_t(attn_w[3], wide(lambda i: attn_q[i])) + bias(3)).astype(BF16).astype(F32)
            for i in range(height):
                y = (feat[0, t, i].astype(F32) + o[:, i * width:(i + 1) * width]).astype(BF16)
                feat[0, t, i] = y
                xres[t, i] = y
            return 0

        lax.fori_loop(0, 2, frame, 0)

    x_copy().start()
    for j in range(4):
        param_copy(j).start()
    start_weights(0)
    param_copy(4).start()
    barrier = pltpu.get_barrier_semaphore()
    for d in range(1, ranks):
        pl.semaphore_signal(barrier, inc=1, device_id={"time": lax.rem(me + d, ranks)}, device_id_type=MESH)
    start_weights(1)
    for s in range(4):
        for row in (0, height + 1):
            u_bufs[s][row] = jnp.zeros((k_tap, width), BF16)
    magic = (65536 + per_group - 1) // per_group
    r = lax.broadcasted_iota(jnp.int32, (channels, channels), 0) * magic // 65536
    c = lax.broadcasted_iota(jnp.int32, (channels, channels), 1) * magic // 65536
    member[...] = jnp.where(r == c, 1.0, 0.0).astype(BF16)
    x_copy().wait()
    for t in range(2):
        for i in range(height):
            x = x_in[t, pl.ds(i * width, width), :].T
            feat[0, t, i] = x
            xres[t, i] = x

    def plain_value(t, c0, i):
        return feat[0, t, i, pl.ds(c0, CHUNK), :].astype(F32)

    accumulate_stats(plain_value)
    for j in range(5):
        param_copy(j).wait()
    pl.semaphore_wait(barrier, ranks - 1)
    send_stats(0)
    start_halo(0)

    def conv_stage(k, _):
        src = k % 2
        dst = 1 - src
        n = k + k // 2
        slot = k % 2
        bias_col[...] = column(conv_b[pl.ds(k, 1), :])
        norm_coefs(n, 0.5)
        fill_u(frame_read(src, 0), 2)
        wait_weights(k, 2)
        wait_weights(k, 1)
        put(acc.at[0], dot_t(weights(slot, 2), taps(2)))
        for c0 in range(0, channels, CHUNK):
            fill_rows(frame_read(src, 1), 3, c0, CHUNK)
        put(acc.at[1], dot_t(weights(slot, 1, 2), jnp.concatenate([taps(2), taps(3)], axis=0)))
        wait_weights(k, 0)
        get_halo(k, 1)
        put(acc.at[1], wide(lambda i: acc[1, i]) + dot_t(weights(slot, 0), taps(1)))
        put(acc.at[0], wide(lambda i: acc[0, i]) + dot_t(weights(slot, 1), taps(1)))
        get_halo(k, 0)

        @pl.when(me < ranks - 1)
        def _():
            for t in (1, 0):
                halo_copy(k, t).wait_send()

        odd = src == 1

        def finish(t, value):
            for c0 in range(0, channels, CHUNK):
                rows = pl.ds(c0, CHUNK)
                s1 = jnp.zeros((CHUNK, width), F32) if t else part[0, rows, :]
                s2 = jnp.zeros((CHUNK, width), F32) if t else part[1, rows, :]
                ys = []
                for i in range(height):
                    h = (value(i, c0) + bias_col[rows, :]).astype(BF16).astype(F32)
                    y = jnp.where(odd, xres[t, i, rows, :].astype(F32) + h, h).astype(BF16)
                    ys.append(y)
                    y = y.astype(F32)
                    s1 = s1 + y
                    s2 = s2 + y * y
                for i in range(height):
                    feat[dst, t, i, rows, :] = ys[i]
                part[0, rows, :] = s1
                part[1, rows, :] = s2

        last = dot_t(weights(slot, 0), taps(0))
        finish(1, lambda i, c0: acc[1, i, pl.ds(c0, CHUNK), :])
        finish(0, lambda i, c0: acc[0, i, pl.ds(c0, CHUNK), :]
               + last[c0:c0 + CHUNK, i * width:(i + 1) * width])

        @pl.when(k < 2)
        def _():
            start_weights(k + 2)

        @pl.when(k < 3)
        def _():
            send_stats(n + 1)

        @pl.when(src == 0)
        def _():
            start_halo(k + 1)

        @pl.when(k == 1)
        def _():
            norm_coefs(2, 1.0)
            attention()
            accumulate_stats(plain_value)
            send_stats(3)
            start_halo(2)

        return 0

    lax.fori_loop(0, 4, conv_stage, 0)
    def out_copy(t):
        return pltpu.make_async_copy(x_in.at[t], out_hbm.at[t], out_sem.at[t])

    for t in (1, 0):
        for i in range(height):
            x_in[t, pl.ds(i * width, width), :] = feat[0, t, i].T
        out_copy(t).start()
    for t in (1, 0):
        out_copy(t).wait()


def solution(mesh):
    ranks = mesh.shape["time"]
    video_spec = P(("batch", "time"), None, None, None)

    def device_body(latent, conv_w, conv_b, norm_g, norm_b, attn_w, attn_b):
        frames, height, width, channels = latent.shape
        npos = height * width
        hbm = pl.BlockSpec(memory_space=pl.ANY)
        dma = pltpu.SemaphoreType.DMA
        out = pl.pallas_call(
            functools.partial(kernel, ranks, height, width),
            out_shape=jax.ShapeDtypeStruct((frames, npos, channels), BF16),
            in_specs=[hbm] * 7,
            out_specs=hbm,
            scratch_shapes=[
                pltpu.VMEM(conv_b.shape, conv_b.dtype),
                pltpu.VMEM(norm_g.shape, norm_g.dtype),
                pltpu.VMEM(norm_b.shape, norm_b.dtype),
                pltpu.VMEM(attn_w.shape, attn_w.dtype),
                pltpu.VMEM(attn_b.shape, attn_b.dtype),
                pltpu.VMEM((frames, npos, channels), BF16),
                pltpu.VMEM((2, 3, channels // 128, 9 * channels, 128), BF16),
                pltpu.VMEM((height + 2, 3 * channels, width), BF16),
                pltpu.VMEM((height + 2, 3 * channels, width), BF16),
                pltpu.VMEM((height + 2, 3 * channels, width), BF16),
                pltpu.VMEM((height + 2, 3 * channels, width), BF16),
                pltpu.VMEM((2, height, channels, width), F32),
                pltpu.VMEM((2, 2, height, channels, width), BF16),
                pltpu.VMEM((2, height, channels, width), BF16),
                pltpu.VMEM((4, 2, height, channels, width), BF16),
                pltpu.VMEM((2, channels, 128), F32),
                pltpu.VMEM((5, ranks, 2, channels), F32),
                pltpu.VMEM((3, channels, 128), F32),
                pltpu.VMEM((channels, 128), F32),
                pltpu.VMEM((channels, channels), BF16),
                pltpu.VMEM((2, height, channels, width), BF16),
                pltpu.VMEM((height, channels, width), BF16),
                pltpu.VMEM((height, channels, width), BF16),
                pltpu.VMEM((height, channels, width), BF16),
                pltpu.VMEM((height, npos, width), BF16),
                dma(()), dma((5,)), dma((2,)), dma((2, 3, channels // 128)), dma((5, ranks)), dma((5, ranks)), dma((4, 2)), dma((4, 2)),
            ],
            compiler_params=pltpu.CompilerParams(
                collective_id=0, has_side_effects=True, vmem_limit_bytes=62 * 2 ** 20),
            name="mid_block",
        )(latent.reshape(frames, npos, channels), conv_w.reshape(4, 3, 9 * channels, channels),
          conv_b, norm_g, norm_b, attn_w, attn_b)
        return out.reshape(latent.shape)

    return jax.shard_map(device_body, mesh=mesh, in_specs=(video_spec, P(), P(), P(), P(), P(), P()),
                         out_specs=video_spec, check_vma=False)
```
